32 devices in a mesh: rep: 4 (over z), fsdp: 8 (over y, x, core).
Axes of the slice: x: 2, y: 2, z: 4, core: 2. Of those that a mesh axis runs over, the one named last changes fastest.
Arguments:
- tokens: bfloat16 [16384, 2048], P(('rep', 'fsdp')), may hold values from -6 to 6
- norm_gain: float32 [2048], replicated, may hold values from 0.5 to 1.5
- outer_params: float32 [2, 2048, 4096], P(None, 'fsdp'), may hold values from -6 to 6
- momentum: float32 [2, 2048, 4096], P(None, 'fsdp'), may hold values from -6 to 6
- deltas: bfloat16 [4, 2, 2048, 4096], P('rep', None, 'fsdp'), may hold values from -6 to 6
Outputs:
- new_params: float32 [2, 2048, 4096], P(None, 'fsdp')
- new_momentum: float32 [2, 2048, 4096], P(None, 'fsdp')
- hidden: bfloat16 [16384, 4096], P(('rep', 'fsdp'))
The draws below stay inside these ranges and needn't reach their ends.
All inputs are finite; a program needn't handle non-finite values.
Results may differ from the reference program's by a relative error of at most 0.01.
Values may be sent and summed in bfloat16 or wider, within the bound.
A program may use at most 192 MiB of HBM per device.

```python
import math
import jax
import jax.numpy as jnp
from jax import lax

D = 2048
FF = 4096
TOKENS = 16384
N_REP = 4


def block_levels(stream_key, shape, split, least, largest):
    def one(position, blocks):
        heights = jax.random.uniform(jax.random.fold_in(jax.random.fold_in(stream_key, 6), position), (blocks,), jnp.float32, least / len(split), largest / len(split))
        return jnp.repeat(jnp.exp(heights), shape[position] // blocks).reshape((-1,) + (1,) * (len(shape) - position - 1))

    loudness = one(*split[0])
    for cut in split[1:]:
        loudness = loudness * one(*cut)
    return loudness


def normal_values(stream_key, dims, deviation, most, pieces=(), held_as=jnp.bfloat16):
    values = jax.random.normal(stream_key, dims, jnp.float32) * deviation
    if len(pieces) > 0:
        values = block_levels(stream_key, dims, pieces, -0.22, 0.18) * values
    return jnp.clip(values, min=-most, max=most).astype(held_as)


def setup_inputs(seed: int = 0) -> dict:
    key_list = jax.random.split(jax.random.key(seed), 6)
    return {
        "tokens": normal_values(key_list[0], (TOKENS, D), 1.0, 6.0, ((0, 32),)),
        "norm_gain": jnp.clip(1.0 + 0.1 * jax.random.normal(key_list[1], (D,), jnp.float32), 0.5, 1.5),
        "outer_params": normal_values(key_list[2], (2, D, FF), 1.0, 6.0, ((1, 8),), jnp.float32),
        "momentum": normal_values(key_list[3], (2, D, FF), 0.5, 6.0, ((1, 8),), jnp.float32),
        "deltas": normal_values(key_list[4], (N_REP, 2, D, FF), 0.5, 6.0, ((0, 4), (2, 8))),
    }


EPS = 1e-05
MU = 0.9
RATE = 0.7

def reference(tokens, norm_gain, outer_params, momentum, deltas):
    total = jnp.zeros(outer_params.shape, jnp.float32)
    for group in range(N_REP):
        total = total + deltas[group].astype(jnp.float32)
    outer_grad = total / N_REP
    new_momentum = MU * momentum + outer_grad
    new_params = outer_params - RATE * (outer_grad + MU * new_momentum)
    weights = new_params.astype(jnp.bfloat16)
    values = tokens.astype(jnp.float32)
    scale_rows = lax.rsqrt(lax.optimization_barrier(jnp.mean(values * values, axis=-1, keepdims=True)) + EPS)
    normed = (values * scale_rows * norm_gain).astype(jnp.bfloat16)
    factor = 1.0 / math.sqrt(D)
    gate = jnp.dot(normed, weights[0], preferred_element_type=jnp.float32) * factor
    up = jnp.dot(normed, weights[1], preferred_element_type=jnp.float32) * factor
    hidden = (jax.nn.silu(gate) * up).astype(jnp.bfloat16)
    return (new_params, new_momentum, hidden)
```

```python
import functools
import math

import jax
import jax.numpy as jnp
from jax import lax
from jax.experimental import pallas as pl
from jax.experimental.pallas import tpu as pltpu
from jax.sharding import PartitionSpec as P

EPS = 1e-05
MU = 0.9
RATE = 0.7
CORES = 2
WIDTH = 256
SUM_LAG = 2
STEP_LAG = 3


def advance(params, moment, summed, groups):
    outer_grad = summed * (1.0 / groups)
    moment_next = MU * moment + outer_grad
    params_next = params - RATE * (outer_grad + MU * moment_next)
    return (params_next, moment_next)


def kernel(
    groups, shards,
    tokens, gain, params, moment, deltas,
    summed, hidden,
    full, own, part_in, peer_in, part, total, normed, p_slots, m_slots, h_slots,
    load_sem, token_sem, pm_sem, out_sem, h_sem,
    part_recv, peer_recv, total_recv, ring_recv, pair_recv,
    part_send, total_send, ring_send, pair_send,
):
    chunks, _, height, width = own.shape
    chips = shards // CORES
    half = chips // 2
    rows = normed.shape[0]
    rep = lax.axis_index("rep")
    mine = lax.axis_index("fsdp")
    core = mine % CORES
    chip = mine // CORES
    turn = half + chips - 1

    def flip(value):
        return value + (value // half) * (turn - 2 * value)

    place = flip(chip)

    def shard_at(position):
        return flip((position + chips) % chips) * CORES + core

    right, left = shard_at(place + 1), shard_at(place - 1)
    partner = chip * CORES + (1 - core)
    middle = groups // 2
    low = rep < middle
    inward = jnp.where(low, rep + 1, rep - 1)
    outward = jnp.where(low, rep - 1, rep + 1)
    at_end = (rep == 0) | (rep == groups - 1)
    at_middle = (rep == middle - 1) | (rep == middle)

    def columns(c):
        return pl.ds(pl.multiple_of(c * width, width), width)

    def block(c, which, owner):
        return full.at[c, which, pl.ds(pl.multiple_of(owner * height, height), height), :]

    def delta_load(c):
        return pltpu.make_async_copy(deltas.at[0, :, :, columns(c)], own.at[c], load_sem.at[c])

    def state_loads(c):
        slot = c % 2
        return (
            pltpu.make_async_copy(params.at[:, :, columns(c)], p_slots.at[slot], pm_sem.at[slot, 0]),
            pltpu.make_async_copy(moment.at[:, :, columns(c)], m_slots.at[slot], pm_sem.at[slot, 1]),
        )

    def part_copy(src, dst, c, recv):
        return pltpu.make_async_remote_copy(
            src_ref=src.at[c], dst_ref=dst.at[c], send_sem=part_send, recv_sem=recv.at[c],
            device_id={"rep": inward}, device_id_type=pl.DeviceIdType.MESH)

    def total_copy(c):
        return pltpu.make_async_remote_copy(
            src_ref=total.at[c], dst_ref=total.at[c], send_sem=total_send, recv_sem=total_recv.at[c],
            device_id={"rep": outward}, device_id_type=pl.DeviceIdType.MESH)

    def ring_copy(c, which, owner, hop, target):
        return pltpu.make_async_remote_copy(
            src_ref=block(c, which, owner), dst_ref=block(c, which, owner),
            send_sem=ring_send.at[which], recv_sem=ring_recv.at[c, which, hop - 1],
            device_id={"fsdp": target}, device_id_type=pl.DeviceIdType.MESH)

    def pair_copy(c, which, owner):
        return pltpu.make_async_remote_copy(
            src_ref=block(c, which, owner), dst_ref=block(c, which, owner),
            send_sem=pair_send, recv_sem=pair_recv.at[c],
            device_id={"fsdp": partner}, device_id_type=pl.DeviceIdType.MESH)

    @pl.loop(0, chunks)
    def _(c):
        delta_load(c).start()

    token_copy = pltpu.make_async_copy(tokens, normed, token_sem)
    token_copy.start()
    for copy in state_loads(0):
        copy.start()

    barrier = pltpu.get_barrier_semaphore()
    for target in (partner, left, right):
        pl.semaphore_signal(barrier, inc=1, device_id={"fsdp": target}, device_id_type=pl.DeviceIdType.MESH)
    pl.semaphore_signal(barrier, inc=1, device_id={"rep": inward}, device_id_type=pl.DeviceIdType.MESH)

    @pl.when(jnp.logical_not(at_end))
    def _():
        pl.semaphore_signal(barrier, inc=1, device_id={"rep": outward}, device_id_type=pl.DeviceIdType.MESH)
        pl.semaphore_wait(barrier, 5)

    @pl.when(at_end)
    def _():
        pl.semaphore_wait(barrier, 4)

    @pl.loop(0, chunks)
    def _(c):
        delta_load(c).wait()

        @pl.when(at_end & jnp.logical_not(at_middle))
        def _():
            part_copy(own, part_in, c, part_recv).start()

        @pl.when(at_end & at_middle)
        def _():
            part_copy(own, peer_in, c, peer_recv).start()

    token_copy.wait()
    piece = 64

    @pl.loop(0, rows // piece)
    def _(i):
        at = pl.ds(pl.multiple_of(i * piece, piece), piece)
        values = normed[at, :].astype(jnp.float32)
        scale = lax.rsqrt(jnp.mean(values * values, axis=-1, keepdims=True) + EPS)
        normed[at, :] = (values * scale * gain[...]).astype(jnp.bfloat16)

    factor = 1.0 / math.sqrt(normed.shape[1])
    last = chips - 1

    def live(c):
        return (c >= 0) & (c < chunks)

    @pl.loop(0, chunks + STEP_LAG + chips)
    def _(t):
        for hop in range(last, 0, -1):
            c = t - STEP_LAG - hop

            @pl.when(live(c))
            def _(c=c, hop=hop):
                for which, owner, target in ((0, shard_at(place - hop), right), (1, shard_at(place + hop), left)):
                    ring_copy(c, which, owner, hop, target).wait_recv()
                    if hop < last:
                        ring_copy(c, which, owner, hop + 1, target).start()
                    pair_copy(c, which, owner).start()

        u = t - STEP_LAG

        @pl.when(live(u))
        def _():
            @pl.when(jnp.logical_not(at_middle))
            def _():
                total_copy(u).wait_recv()

                @pl.when(jnp.logical_not(at_end))
                def _():
                    total_copy(u).start()

            @pl.when(u + 1 < chunks)
            def _():
                for copy in state_loads(u + 1):
                    copy.start()

            for copy in state_loads(u):
                copy.wait()
            slot = u % 2
            at = pl.ds(pl.multiple_of(mine * height, height), height)
            for which, target in ((0, right), (1, left)):
                stepped, _ = advance(
                    p_slots[slot, which], m_slots[slot, which], total[u, which].astype(jnp.float32), groups)
                full[u, which, at, :] = stepped.astype(jnp.bfloat16)
                ring_copy(u, which, mine, 1, target).start()
                pair_copy(u, which, mine).start()
            pltpu.make_async_copy(total.at[u], summed.at[:, :, columns(u)], out_sem).start()

        s = t - SUM_LAG

        @pl.when(live(s) & at_middle)
        def _():
            part_copy(part, peer_in, s, peer_recv).wait_recv()

            @pl.when(at_end)
            def _():
                total[s] = (own[s].astype(jnp.float32) + peer_in[s].astype(jnp.float32)).astype(jnp.bfloat16)

            @pl.when(jnp.logical_not(at_end))
            def _():
                total[s] = (part[s].astype(jnp.float32) + peer_in[s].astype(jnp.float32)).astype(jnp.bfloat16)
                total_copy(s).start()

        @pl.when((t < chunks) & jnp.logical_not(at_end))
        def _():
            part_copy(part, part_in, t, part_recv).wait_recv()
            part[t] = (own[t].astype(jnp.float32) + part_in[t].astype(jnp.float32)).astype(jnp.bfloat16)

            @pl.when(at_middle)
            def _():
                part_copy(part, peer_in, t, peer_recv).start()

            @pl.when(jnp.logical_not(at_middle))
            def _():
                part_copy(part, part_in, t, part_recv).start()

        c = t - STEP_LAG - chips

        @pl.when(live(c))
        def _():
            arrived = full.at[c, :, 0:chips * height, :]
            pltpu.make_async_copy(arrived, arrived, pair_recv.at[c]).wait()
            slot = c % 2

            @pl.when(c >= 2)
            def _():
                pltpu.make_async_copy(h_slots.at[slot], hidden.at[:, columns(c)], h_sem.at[slot]).wait()

            tall = rows // 2

            @pl.loop(0, 2)
            def _(i):
                at = pl.ds(pl.multiple_of(i * tall, tall), tall)
                gate = jnp.dot(normed[at, :], full[c, 0], preferred_element_type=jnp.float32) * factor
                up = jnp.dot(normed[at, :], full[c, 1], preferred_element_type=jnp.float32) * factor
                h_slots[slot, at, :] = (gate / (1.0 + jnp.exp(-gate)) * up).astype(jnp.bfloat16)

            pltpu.make_async_copy(h_slots.at[slot], hidden.at[:, columns(c)], h_sem.at[slot]).start()

    for slot in range(2):
        pltpu.make_async_copy(h_slots.at[slot], hidden.at[:, columns(0)], h_sem.at[slot]).wait()
    pltpu.make_async_copy(own, own, part_send).wait()
    pltpu.make_async_copy(total, total, out_sem).wait()

    @pl.when(jnp.logical_not(at_end))
    def _():
        pltpu.make_async_copy(total, total, total_send).wait()

    for which in range(2):
        sent = full.at[:, which, 0:last * height, :]
        pltpu.make_async_copy(sent, sent, ring_send.at[which]).wait()
    sent = full.at[:, :, 0:chips * height, :]
    pltpu.make_async_copy(sent, sent, pair_send).wait()


def solution(mesh):
    groups, shards = mesh.shape["rep"], mesh.shape["fsdp"]
    chips = shards // CORES

    def body(tokens, norm_gain, outer_params, momentum, deltas):
        rows, model = tokens.shape
        _, height, hid = outer_params.shape
        width = WIDTH
        chunks = hid // width
        bf16, f32 = jnp.bfloat16, jnp.float32
        dma = pltpu.SemaphoreType.DMA
        strip = pltpu.VMEM((chunks, 2, height, width), bf16)
        anywhere = pl.BlockSpec(memory_space=pl.ANY)
        summed, hidden = pl.pallas_call(
            functools.partial(kernel, groups, shards),
            out_shape=(
                jax.ShapeDtypeStruct(outer_params.shape, bf16),
                jax.ShapeDtypeStruct((rows, hid), bf16),
            ),
            in_specs=[anywhere, pl.BlockSpec(memory_space=pltpu.VMEM), anywhere, anywhere, anywhere],
            out_specs=(anywhere, anywhere),
            scratch_shapes=[
                pltpu.VMEM((chunks, 2, model, width), bf16),
                strip, strip, strip, strip, strip,
                pltpu.VMEM((rows, model), bf16),
                pltpu.VMEM((2, 2, height, width), f32),
                pltpu.VMEM((2, 2, height, width), f32),
                pltpu.VMEM((2, rows, width), bf16),
                dma((chunks,)), dma, dma((2, 2)), dma, dma((2,)),
                dma((chunks,)), dma((chunks,)), dma((chunks,)), dma((chunks, 2, chips - 1)), dma((chunks,)),
                dma, dma, dma((2,)), dma,
            ],
            compiler_params=pltpu.CompilerParams(
                collective_id=0, has_side_effects=True, vmem_limit_bytes=62 * 1024 * 1024),
            name="round",
        )(tokens, norm_gain.reshape(1, model), outer_params, momentum, deltas)
        new_params, new_momentum = advance(outer_params, momentum, summed.astype(f32), groups)
        return (new_params, new_momentum, hidden)

    in_specs = (
        P(("rep", "fsdp"), None),
        P(),
        P(None, "fsdp", None),
        P(None, "fsdp", None),
        P("rep", None, "fsdp", None),
    )
    out_specs = (P(None, "fsdp", None), P(None, "fsdp", None), P(("rep", "fsdp"), None))
    return jax.shard_map(body, mesh=mesh, in_specs=in_specs, out_specs=out_specs, check_vma=False)
```

```python
import functools
import math

import jax
import jax.numpy as jnp
from jax import lax
from jax.experimental import pallas as pl
from jax.experimental.pallas import tpu as pltpu
from jax.sharding import PartitionSpec as P

EPS = 1e-05
MU = 0.9
RATE = 0.7
CORES = 2
WIDTH = 256
SUM_LAG = 1
STEP_LAG = 2
SPLIT = 2


def advance(params, moment, summed, groups):
    outer_grad = summed * (1.0 / groups)
    moment_next = MU * moment + outer_grad
    params_next = params - RATE * (outer_grad + MU * moment_next)
    return (params_next, moment_next)


def kernel(
    groups, shards,
    tokens, gain, params, moment, deltas,
    p_out, m_out, hidden,
    full, own, peer_in, total, normed, h_slots,
    load_sem, token_sem, pm_sem, h_sem,
    part_recv, peer_recv, total_recv, ring_recv, pair_recv,
    part_send, total_send, ring_send, pair_send,
):
    chunks, pieces, low_height, width = own.shape
    split = pieces // 2
    height = low_height * split
    chips = shards // CORES
    half = chips // 2
    rows = normed.shape[0]
    rep = lax.axis_index("rep")
    mine = lax.axis_index("fsdp")
    core = mine % CORES
    chip = mine // CORES
    turn = half + chips - 1

    def flip(value):
        return value + (value // half) * (turn - 2 * value)

    place = flip(chip)

    def shard_at(position):
        return flip((position + chips) % chips) * CORES + core

    right, left = shard_at(place + 1), shard_at(place - 1)
    partner = chip * CORES + (1 - core)
    middle = groups // 2
    low = rep < middle
    inward = jnp.where(low, rep + 1, rep - 1)
    outward = jnp.where(low, rep - 1, rep + 1)
    at_end = (rep == 0) | (rep == groups - 1)
    at_middle = (rep == middle - 1) | (rep == middle)

    def columns(c):
        return pl.ds(pl.multiple_of(c * width, width), width)

    def block(c, which, owner):
        return full.at[c, which, pl.ds(pl.multiple_of(owner * height, height), height), :]

    def delta_load(c, q):
        at = pl.ds((q % split) * low_height, low_height)
        return pltpu.make_async_copy(deltas.at[0, q // split, at, columns(c)], own.at[c, q], load_sem.at[c])

    def state_loads(c):
        return (
            pltpu.make_async_copy(params.at[:, :, columns(c)], p_out.at[:, :, columns(c)], pm_sem.at[c % 2, 0]),
            pltpu.make_async_copy(moment.at[:, :, columns(c)], m_out.at[:, :, columns(c)], pm_sem.at[c % 2, 1]),
        )

    def part_copy(dst, c, q, recv):
        return pltpu.make_async_remote_copy(
            src_ref=own.at[c, q], dst_ref=dst.at[c, q], send_sem=part_send, recv_sem=recv.at[c, q],
            device_id={"rep": inward}, device_id_type=pl.DeviceIdType.MESH)

    def total_copy(c, q):
        return pltpu.make_async_remote_copy(
            src_ref=total.at[c, q], dst_ref=total.at[c, q], send_sem=total_send, recv_sem=total_recv.at[c, q],
            device_id={"rep": outward}, device_id_type=pl.DeviceIdType.MESH)

    def ring_copy(c, which, owner, hop, target):
        return pltpu.make_async_remote_copy(
            src_ref=block(c, which, owner), dst_ref=block(c, which, owner),
            send_sem=ring_send.at[which], recv_sem=ring_recv.at[c, which, hop - 1],
            device_id={"fsdp": target}, device_id_type=pl.DeviceIdType.MESH)

    def pair_copy(c, which, owner):
        return pltpu.make_async_remote_copy(
            src_ref=block(c, which, owner), dst_ref=block(c, which, owner),
            send_sem=pair_send, recv_sem=pair_recv.at[c],
            device_id={"fsdp": partner}, device_id_type=pl.DeviceIdType.MESH)

    @pl.loop(0, chunks)
    def _(c):
        for q in range(pieces):
            delta_load(c, q).start()

    token_copy = pltpu.make_async_copy(tokens, normed, token_sem)
    token_copy.start()
    for copy in state_loads(0):
        copy.start()

    barrier = pltpu.get_barrier_semaphore()
    for target in (partner, left, right):
        pl.semaphore_signal(barrier, inc=1, device_id={"fsdp": target}, device_id_type=pl.DeviceIdType.MESH)
    pl.semaphore_signal(barrier, inc=1, device_id={"rep": inward}, device_id_type=pl.DeviceIdType.MESH)

    @pl.when(jnp.logical_not(at_end))
    def _():
        pl.semaphore_signal(barrier, inc=1, device_id={"rep": outward}, device_id_type=pl.DeviceIdType.MESH)
        pl.semaphore_wait(barrier, 5)

    @pl.when(at_end)
    def _():
        pl.semaphore_wait(barrier, 4)

    @pl.loop(0, chunks)
    def _(c):
        pltpu.make_async_copy(own.at[c], own.at[c], load_sem.at[c]).wait()

        @pl.when(at_end & jnp.logical_not(at_middle))
        def _():
            for q in range(pieces):
                part_copy(total, c, q, part_recv).start()

        @pl.when(at_end & at_middle)
        def _():
            for q in range(pieces):
                part_copy(peer_in, c, q, peer_recv).start()

    token_copy.wait()
    piece = 64

    @pl.loop(0, rows // piece)
    def _(i):
        at = pl.ds(pl.multiple_of(i * piece, piece), piece)
        values = normed[at, :].astype(jnp.float32)
        scale = lax.rsqrt(jnp.mean(values * values, axis=-1, keepdims=True) + EPS)
        normed[at, :] = (values * scale * gain[...]).astype(jnp.bfloat16)

    factor = 1.0 / math.sqrt(normed.shape[1])
    last = chips - 1

    def live(c):
        return (c >= 0) & (c < chunks)

    @pl.loop(0, chunks + STEP_LAG + chips)
    def _(t):
        for hop in range(last, 0, -1):
            c = t - STEP_LAG - hop

            @pl.when(live(c))
            def _(c=c, hop=hop):
                for which, owner, target in ((0, shard_at(place - hop), right), (1, shard_at(place + hop), left)):
                    ring_copy(c, which, owner, hop, target).wait_recv()
                    if hop < last:
                        ring_copy(c, which, owner, hop + 1, target).start()
                    pair_copy(c, which, owner).start()

        u = t - STEP_LAG

        @pl.when(live(u))
        def _():
            @pl.when(u + 1 < chunks)
            def _():
                for copy in state_loads(u + 1):
                    copy.start()

            for copy in state_loads(u):
                copy.wait()
            for which, target in ((0, right), (1, left)):
                @pl.when(jnp.logical_not(at_middle))
                def _(which=which):
                    for q in range(which * split, (which + 1) * split):
                        total_copy(u, q).wait_recv()

                        @pl.when(jnp.logical_not(at_end))
                        def _(q=q):
                            total_copy(u, q).start()

                for q in range(which * split, (which + 1) * split):
                    rows_here = slice((q % split) * low_height, (q % split + 1) * low_height)
                    stepped, moved = advance(
                        p_out[which, rows_here, columns(u)], m_out[which, rows_here, columns(u)],
                        total[u, q].astype(jnp.float32), groups)
                    p_out[which, rows_here, columns(u)] = stepped
                    m_out[which, rows_here, columns(u)] = moved
                    start = mine * height + (q % split) * low_height
                    at = pl.ds(pl.multiple_of(start, low_height), low_height)
                    full[u, which, at, :] = stepped.astype(jnp.bfloat16)
                ring_copy(u, which, mine, 1, target).start()
                pair_copy(u, which, mine).start()

        s = t - SUM_LAG

        @pl.when(live(s) & at_middle)
        def _():
            for q in range(pieces):
                part_copy(peer_in, s, q, peer_recv).wait_recv()
                total[s, q] = (own[s, q].astype(jnp.float32) + peer_in[s, q].astype(jnp.float32)).astype(jnp.bfloat16)

                @pl.when(jnp.logical_not(at_end))
                def _(q=q):
                    total_copy(s, q).start()

        @pl.when((t < chunks) & jnp.logical_not(at_end))
        def _():
            for q in range(pieces):
                part_copy(total, t, q, part_recv).wait_recv()
                own[t, q] = (own[t, q].astype(jnp.float32) + total[t, q].astype(jnp.float32)).astype(jnp.bfloat16)

                @pl.when(at_middle)
                def _(q=q):
                    part_copy(peer_in, t, q, peer_recv).start()

                @pl.when(jnp.logical_not(at_middle))
                def _(q=q):
                    part_copy(total, t, q, part_recv).start()

        c = t - STEP_LAG - chips

        @pl.when(live(c))
        def _():
            arrived = full.at[c, :, 0:chips * height, :]
            pltpu.make_async_copy(arrived, arrived, pair_recv.at[c]).wait()
            slot = c % 2

            @pl.when(c >= 2)
            def _():
                pltpu.make_async_copy(h_slots.at[slot], hidden.at[:, columns(c)], h_sem.at[slot]).wait()

            tall = rows // 2

            @pl.loop(0, 2)
            def _(i):
                at = pl.ds(pl.multiple_of(i * tall, tall), tall)
                gate = jnp.dot(normed[at, :], full[c, 0], preferred_element_type=jnp.float32) * factor
                up = jnp.dot(normed[at, :], full[c, 1], preferred_element_type=jnp.float32) * factor
                h_slots[slot, at, :] = (gate / (1.0 + jnp.exp(-gate)) * up).astype(jnp.bfloat16)

            pltpu.make_async_copy(h_slots.at[slot], hidden.at[:, columns(c)], h_sem.at[slot]).start()

    for slot in range(2):
        pltpu.make_async_copy(h_slots.at[slot], hidden.at[:, columns(0)], h_sem.at[slot]).wait()
    pltpu.make_async_copy(own, own, part_send).wait()

    @pl.when(jnp.logical_not(at_end))
    def _():
        pltpu.make_async_copy(total, total, total_send).wait()

    for which in range(2):
        sent = full.at[:, which, 0:last * height, :]
        pltpu.make_async_copy(sent, sent, ring_send.at[which]).wait()
    sent = full.at[:, :, 0:chips * height, :]
    pltpu.make_async_copy(sent, sent, pair_send).wait()


def solution(mesh):
    groups, shards = mesh.shape["rep"], mesh.shape["fsdp"]
    chips = shards // CORES

    def body(tokens, norm_gain, outer_params, momentum, deltas):
        rows, model = tokens.shape
        _, height, hid = outer_params.shape
        width = WIDTH
        chunks = hid // width
        bf16, f32 = jnp.bfloat16, jnp.float32
        dma = pltpu.SemaphoreType.DMA
        strip = pltpu.VMEM((chunks, 2 * SPLIT, height // SPLIT, width), bf16)
        each = dma((chunks, 2 * SPLIT))
        anywhere = pl.BlockSpec(memory_space=pl.ANY)
        new_params, new_momentum, hidden = pl.pallas_call(
            functools.partial(kernel, groups, shards),
            out_shape=(
                pltpu.VMEM(outer_params.shape, f32),
                pltpu.VMEM(outer_params.shape, f32),
                jax.ShapeDtypeStruct((rows, hid), bf16),
            ),
            in_specs=[anywhere, pl.BlockSpec(memory_space=pltpu.VMEM), anywhere, anywhere, anywhere],
            out_specs=(pl.BlockSpec(memory_space=pltpu.VMEM), pl.BlockSpec(memory_space=pltpu.VMEM), anywhere),
            scratch_shapes=[
                pltpu.VMEM((chunks, 2, model, width), bf16),
                strip, strip, strip,
                pltpu.VMEM((rows, model), bf16),
                pltpu.VMEM((2, rows, width), bf16),
                dma((chunks,)), dma, dma((2, 2)), dma((2,)),
                each, each, each, dma((chunks, 2, chips - 1)), dma((chunks,)),
                dma, dma, dma((2,)), dma,
            ],
            compiler_params=pltpu.CompilerParams(
                collective_id=0, has_side_effects=True, vmem_limit_bytes=191 * 256 * 1024),
            name="round",
        )(tokens, norm_gain.reshape(1, model), outer_params, momentum, deltas)
        return (new_params, new_momentum, hidden)

    in_specs = (
        P(("rep", "fsdp"), None),
        P(),
        P(None, "fsdp", None),
        P(None, "fsdp", None),
        P("rep", None, "fsdp", None),
    )
    out_specs = (P(None, "fsdp", None), P(None, "fsdp", None), P(("rep", "fsdp"), None))
    return jax.shard_map(body, mesh=mesh, in_specs=in_specs, out_specs=out_specs, check_vma=False)
```
